32 devices in a mesh: member: 8 (over y, x, core), lat: 4 (over z).
Axes of the slice: x: 2, y: 2, z: 4, core: 2. Of those that a mesh axis runs over, the one named last changes fastest.
Arguments:
- starting_state_array: bfloat16 [8, 640, 4, 2560], P('member', 'lat'), may hold values from -6 to 6
- stochastic_forcing_array: bfloat16 [8, 640, 4, 2560], P('member', 'lat'), may hold values from -2 to 2
- decoded_outlook_array: bfloat16 [8, 640, 4, 2560], P('member', 'lat'), may hold values from -6 to 6
- truth_analysis_array: bfloat16 [640, 4, 2560], P('lat'), may hold values from -6 to 6
- weighted_polynomial_basis: bfloat16 [320, 640, 320], P('lat'), may hold values from -0.25 to 0.25
- wavenumber_attenuation: float32 [320], replicated, may hold values from 0.05 to 0.5
Outputs:
- advanced: bfloat16 [8, 640, 4, 2560], P('member', 'lat')
- adjoint: bfloat16 [8, 640, 4, 2560], P('member', 'lat')
The draws below stay inside these ranges and needn't reach their ends.
All inputs are finite; a program needn't handle non-finite values.
Results may differ from the reference program's by a relative error of at most 0.0081.
Values may be sent and summed in bfloat16 or wider, within the bound.
No kernel may reach another device: no remote copies, remote signals or barrier semaphores. Data moves between devices by JAX's collectives and lax.ppermute only.
A program may use at most 192 MiB of HBM per device.

```python
import math
import jax
import jax.numpy as jnp
from jax import lax

GRID_BAND_TALLY = 640
STRATUM_TALLY = 4
EASTWARD_TALLY = 2560
KM = 320
NDEG = 320
TRAJECTORY_TALLY = 8


def levels(rng, shape, pieces, least, high):
    def one(dim, parts):
        steps = jax.random.uniform(jax.random.fold_in(jax.random.fold_in(rng, 6), dim), (parts,), jnp.float32, least / len(pieces), high / len(pieces))
        return jnp.repeat(jnp.exp(steps), shape[dim] // parts).reshape((-1,) + (1,) * (len(shape) - dim - 1))

    level = one(*pieces[0])
    for cut in pieces[1:]:
        level = level * one(*cut)
    return level


def scatter_about(stream_key, shape, spread, bound, split=(), held_as=jnp.bfloat16):
    result = spread * jax.random.normal(stream_key, shape, jnp.float32)
    if split:
        result = result * levels(stream_key, shape, split, -0.22, 0.18)
    return jnp.clip(result, -bound, bound).astype(held_as)


def setup_inputs(seed: int = 0) -> dict:
    arg_keys = jax.random.split(jax.random.key(seed), 7)
    starting_state_array = scatter_about(arg_keys[0], (TRAJECTORY_TALLY, GRID_BAND_TALLY, STRATUM_TALLY, EASTWARD_TALLY), 1.0, 6.0, ((0, 8), (1, 4)))
    stochastic_forcing_array = scatter_about(arg_keys[1], (TRAJECTORY_TALLY, GRID_BAND_TALLY, STRATUM_TALLY, EASTWARD_TALLY), 0.3, 2.0, ((0, 8), (1, 4)))
    decoded_outlook_array = scatter_about(arg_keys[2], (TRAJECTORY_TALLY, GRID_BAND_TALLY, STRATUM_TALLY, EASTWARD_TALLY), 1.0, 6.0, ((0, 8), (1, 4)))
    truth_analysis_array = scatter_about(arg_keys[3], (GRID_BAND_TALLY, STRATUM_TALLY, EASTWARD_TALLY), 1.0, 6.0, ((0, 4),))
    weighted_polynomial_basis = scatter_about(arg_keys[4], (KM, GRID_BAND_TALLY, NDEG), GRID_BAND_TALLY ** -0.5, 0.25, ((0, 4),))
    wavenumber_attenuation = jnp.clip(jnp.exp(jax.random.uniform(arg_keys[5], (NDEG,), jnp.float32, math.log(0.05), math.log(0.5))), 0.05, 0.5)
    return dict(starting_state_array=starting_state_array, stochastic_forcing_array=stochastic_forcing_array, decoded_outlook_array=decoded_outlook_array, truth_analysis_array=truth_analysis_array, weighted_polynomial_basis=weighted_polynomial_basis, wavenumber_attenuation=wavenumber_attenuation)


def fourier_table(lon, waves):
    cols = lax.broadcasted_iota(jnp.int32, (lon, 2 * waves), 1)
    rows = lax.broadcasted_iota(jnp.int32, (lon, 2 * waves), 0)
    wave = cols // 2
    phase = (wave * rows % lon).astype(jnp.float32) * (2.0 * math.pi / lon)
    value = jnp.where(cols % 2 == 0, jnp.cos(phase), jnp.sin(phase))
    return (value * math.sqrt(2.0 / lon)).astype(jnp.bfloat16)

def spectral_filter(field, table, weighted_polynomial_basis, wavenumber_attenuation):
    coeffs = jnp.dot(field.reshape(GRID_BAND_TALLY * STRATUM_TALLY, EASTWARD_TALLY), table, preferred_element_type=jnp.float32)
    coeffs = coeffs.astype(jnp.bfloat16).reshape(GRID_BAND_TALLY, STRATUM_TALLY, KM, 2)
    spectra = jnp.einsum('mln,lemp->mnep', weighted_polynomial_basis.astype(jnp.float32), coeffs.astype(jnp.float32))
    spectra = (spectra * wavenumber_attenuation[None, :, None, None]).astype(jnp.bfloat16)
    synthesis = jnp.einsum('mln,mnep->lemp', weighted_polynomial_basis.astype(jnp.float32), spectra.astype(jnp.float32))
    synthesis = synthesis.astype(jnp.bfloat16).reshape(GRID_BAND_TALLY * STRATUM_TALLY, 2 * KM)
    grid = jnp.dot(synthesis, table.T, preferred_element_type=jnp.float32)
    return grid.reshape(GRID_BAND_TALLY, STRATUM_TALLY, EASTWARD_TALLY)

def reference(starting_state_array, stochastic_forcing_array, decoded_outlook_array, truth_analysis_array, weighted_polynomial_basis, wavenumber_attenuation):
    table = fourier_table(EASTWARD_TALLY, KM)
    trajectory_items = decoded_outlook_array.astype(jnp.float32)
    sorted_positions = lax.map(lambda single: lax.optimization_barrier(jnp.sum(jnp.sign(single[None] - trajectory_items), axis=0)), trajectory_items)
    score_derivative = (jnp.sign(trajectory_items - truth_analysis_array.astype(jnp.float32)[None]) - sorted_positions / (TRAJECTORY_TALLY - 1)).astype(jnp.bfloat16)
    advanced = lax.map(lambda single: spectral_filter(single, table, weighted_polynomial_basis, wavenumber_attenuation), starting_state_array)
    adjoint = lax.map(lambda single: spectral_filter(single, table, weighted_polynomial_basis, wavenumber_attenuation), score_derivative)
    advanced = (advanced + stochastic_forcing_array.astype(jnp.float32)).astype(jnp.bfloat16)
    return (advanced, adjoint.astype(jnp.bfloat16))
```

```python
import math

import jax
import jax.numpy as jnp
from jax import lax
from jax.experimental import pallas as pl
from jax.experimental.pallas import tpu as pltpu
from jax.sharding import PartitionSpec as P


def wave_trig(wave, place, lon):
    phase = (wave * place % lon).astype(jnp.float32) * (2.0 * math.pi / lon)
    return jnp.cos(phase), jnp.sin(phase)


def fourier_rows(lon, lat, member, per, waves):
    fine = math.gcd(lon, 128)
    row = lax.broadcasted_iota(jnp.int32, (lat.shape[0], per * 2, 1), 1)
    part = (row % 2).reshape(-1, 1)
    place = (member[:, None, None] * per + row // 2).reshape(-1, 1)
    wave = place + jnp.repeat(lat * waves, per * 2)[:, None]
    rows = wave.shape[0]
    scale = jnp.where(place < waves, math.sqrt(2.0 / lon), 0.0)
    cos_a, sin_a = wave_trig(wave, lax.broadcasted_iota(jnp.int32, (1, lon // fine), 1) * fine, lon)
    cos_b, sin_b = wave_trig(wave, lax.broadcasted_iota(jnp.int32, (1, fine), 1), lon)
    first = jnp.where(part == 0, cos_a, sin_a) * scale
    second = jnp.where(part == 0, -sin_a, cos_a) * scale
    first, second, cos_b, sin_b = lax.optimization_barrier((first, second, cos_b, sin_b))
    value = first[:, :, None] * cos_b[:, None, :] + second[:, :, None] * sin_b[:, None, :]
    return lax.optimization_barrier(value.reshape(rows, lon).astype(jnp.bfloat16))


def score_kernel(members, slots_ref, *refs):
    truth_ref, table_ref, out_ref, lines_ref = refs[members:]
    step, lon = truth_ref.shape
    padded = lines_ref.shape[0] // members
    inverse = 1.0 / (members - 1)
    lanes = 256 if lon % 256 == 0 else lon
    row = pl.program_id(0) * step
    one, minus, zero = (jnp.full((step, lanes), v, jnp.bfloat16) for v in (1, -1, 0))

    def sign(a, b):
        return jnp.where(a > b, one, jnp.where(a < b, minus, zero))

    def columns(c, carry):
        cols = pl.ds(pl.multiple_of(c * lanes, lanes), lanes)
        values = [refs[i][:, cols] for i in range(members)]
        truth = truth_ref[:, cols]
        ranks = [zero] * members
        for i in range(members):
            for j in range(i):
                s = sign(values[i], values[j])
                ranks[i] = ranks[i] + s
                ranks[j] = ranks[j] - s
        for i in range(members):
            grad = sign(values[i], truth).astype(jnp.float32)
            grad = grad - ranks[i].astype(jnp.float32) * inverse
            place = pl.multiple_of(slots_ref[i] * padded + row, 16)
            lines_ref[pl.ds(place, step), cols] = grad.astype(jnp.bfloat16)
        return carry

    lax.fori_loop(0, lon // lanes, columns, 0)

    @pl.when(pl.program_id(0) == pl.num_programs(0) - 1)
    def _():
        coeffs = lax.dot_general(
            table_ref[...],
            lines_ref[...],
            (((1,), (1,)), ((), ())),
            preferred_element_type=jnp.float32,
        )
        out_ref[...] = coeffs.astype(jnp.bfloat16)


def score_coeffs(blocks, slots, truth, table):
    members = len(blocks)
    piece, lon = truth.shape
    cols = table.shape[0]
    step = 16 if piece % 16 == 0 else piece
    padded = -(-piece // 16) * 16
    spec = pl.BlockSpec((step, lon), lambda i, s: (i, 0))
    coeffs = pl.pallas_call(
        lambda *refs: score_kernel(members, *refs),
        out_shape=jax.ShapeDtypeStruct((cols, members * padded), jnp.bfloat16),
        grid_spec=pltpu.PrefetchScalarGridSpec(
            num_scalar_prefetch=1,
            grid=(piece // step,),
            in_specs=[spec] * (members + 1) + [pl.BlockSpec((cols, lon), lambda i, s: (0, 0))],
            out_specs=pl.BlockSpec((cols, members * padded), lambda i, s: (0, 0)),
            scratch_shapes=[pltpu.VMEM((members * padded, lon), jnp.bfloat16)],
        ),
        compiler_params=pltpu.CompilerParams(vmem_limit_bytes=40 * 2**20),
        name="score",
    )(slots, *blocks, truth, table)
    coeffs = coeffs.reshape(cols, members, padded)[:, :, :piece]
    return coeffs.reshape(cols, members * piece)


def grid_kernel(rows, levels, coeffs_ref, table_ref, *refs):
    out_ref, lines_ref = refs[-2:]
    lines = rows * levels

    @pl.when(pl.program_id(0) == 0)
    def _():
        to = lax.broadcasted_iota(jnp.int32, (lines, lines), 0)
        at = lax.broadcasted_iota(jnp.int32, (lines, lines), 1)
        move = (to % levels * rows + to // levels == at).astype(jnp.bfloat16)
        moved = lax.dot_general(
            move, coeffs_ref[...], (((1,), (1,)), ((), ())), preferred_element_type=jnp.float32
        )
        lines_ref[...] = moved.astype(jnp.bfloat16)

    grid = jnp.dot(lines_ref[...], table_ref[...], preferred_element_type=jnp.float32)
    grid = grid.reshape(rows, levels, -1)
    if len(refs) == 3:
        grid = grid + refs[0][...].astype(jnp.float32)
    out_ref[...] = grid.astype(jnp.bfloat16)


def to_grid(coeffs, table, added, rows, levels):
    cols, lon = table.shape
    step = 512 if lon % 512 == 0 else lon
    block = pl.BlockSpec((rows, levels, step), lambda i: (0, 0, i))
    return pl.pallas_call(
        lambda *refs: grid_kernel(rows, levels, *refs),
        out_shape=jax.ShapeDtypeStruct((rows, levels, lon), jnp.bfloat16),
        grid=(lon // step,),
        in_specs=[
            pl.BlockSpec((cols, rows * levels), lambda i: (0, 0)),
            pl.BlockSpec((cols, step), lambda i: (0, i)),
        ]
        + [block] * (added is not None),
        out_specs=block,
        scratch_shapes=[pltpu.VMEM((rows * levels, cols), jnp.bfloat16)],
        name="grid",
    )(coeffs.reshape(cols, rows * levels), table, *([added] if added is not None else []))


def solution(mesh):
    members, lats = mesh.shape["member"], mesh.shape["lat"]
    both = ("lat", "member")

    def work(start, forcing, outlook, truth, basis, attenuation):
        _, rows, levels, lon = start.shape
        waves, lat_rows, _ = basis.shape
        per = -(-waves // members)
        halves = members // levels
        piece = rows // halves
        me = lax.axis_index("member")

        by_level = outlook[0].transpose(1, 0, 2).reshape(members, piece, lon)
        by_level = lax.optimization_barrier(by_level)
        sent = [lax.dynamic_index_in_dim(by_level, me ^ s, 0, False) for s in range(members)]
        sent, start = lax.optimization_barrier((sent, start))
        blocks, slots = [sent[0]], [me]
        for s in range(1, members):
            blocks.append(
                lax.ppermute(sent[s], "member", [(a, a ^ s) for a in range(members)])
            )
            slots.append(me ^ s)
        truth_here = lax.dynamic_slice(
            truth, (me % halves * piece, me // halves, 0), (piece, 1, lon)
        ).reshape(piece, lon)

        owner = jnp.arange(lats * members)
        table = fourier_rows(lon, owner // members, owner % members, per, waves)
        mine = jnp.pad(basis, ((0, members * per - waves), (0, 0), (0, 0)))
        mine = lax.dynamic_slice_in_dim(mine, me * per, per, 0)

        def lines_coeffs(lines):
            coeffs = lax.dot_general(
                table, lines, (((1,), (1,)), ((), ())), preferred_element_type=jnp.float32
            ).astype(jnp.bfloat16)
            return coeffs

        def to_waves(coeffs):
            coeffs = coeffs.reshape(lats * members, per // 2, 4, -1)
            return lax.all_to_all(coeffs, both, 0, 0, tiled=True)

        def legendre(coeffs):
            spectra = jnp.einsum(
                "jln,jcl->jcn", mine, coeffs, preferred_element_type=jnp.float32
            )
            spectra = (spectra * attenuation).astype(jnp.bfloat16)
            back = jnp.einsum(
                "jln,jcn->jcl", mine, spectra, preferred_element_type=jnp.float32
            ).astype(jnp.bfloat16)
            back = back.reshape(per, members, levels, 2, lats, rows)
            back = back.transpose(4, 1, 0, 3, 2, 5)
            return back.reshape(lats * members, per // 2, 4, levels * rows)

        lines = start[0].transpose(1, 0, 2).reshape(levels * rows, lon)
        received = to_waves(lines_coeffs(lines))
        score = score_coeffs(blocks, jnp.stack(slots), truth_here, table)
        received, score = lax.optimization_barrier((received, score))
        score = to_waves(score)
        coeffs = received.reshape(lats, members, per, 2, levels, rows)
        coeffs = coeffs.transpose(2, 1, 4, 3, 0, 5).reshape(per, members * levels * 2, lat_rows)
        state = to_waves(legendre(coeffs))

        coeffs = score.reshape(lats, levels, halves, per, 2, members, piece)
        coeffs = coeffs.transpose(3, 5, 1, 4, 0, 2, 6)
        coeffs = coeffs.reshape(per, members * levels * 2, lat_rows)
        score = to_waves(legendre(coeffs))
        advanced = to_grid(state, table, forcing[0], rows, levels)
        carried = to_grid(score, table, None, rows, levels)
        return advanced[None], carried[None]

    return jax.shard_map(
        work,
        mesh=mesh,
        in_specs=(
            P("member", "lat", None, None),
            P("member", "lat", None, None),
            P("member", "lat", None, None),
            P("lat", None, None),
            P("lat", None, None),
            P(),
        ),
        out_specs=(P("member", "lat", None, None), P("member", "lat", None, None)),
        check_vma=False,
    )
```

```python
import math

import jax
import jax.numpy as jnp
from jax import lax
from jax.experimental import pallas as pl
from jax.experimental.pallas import tpu as pltpu
from jax.sharding import PartitionSpec as P


def wave_trig(wave, place, lon):
    phase = (wave * place % lon).astype(jnp.float32) * (2.0 * math.pi / lon)
    return jnp.cos(phase), jnp.sin(phase)


def fourier_rows(lon, lat, member, per, waves):
    fine = math.gcd(lon, 128)
    row = lax.broadcasted_iota(jnp.int32, (lat.shape[0], per * 2, 1), 1)
    part = (row % 2).reshape(-1, 1)
    place = (member[:, None, None] * per + row // 2).reshape(-1, 1)
    wave = place + jnp.repeat(lat * waves, per * 2)[:, None]
    rows = wave.shape[0]
    scale = jnp.where(place < waves, math.sqrt(2.0 / lon), 0.0)
    cos_a, sin_a = wave_trig(wave, lax.broadcasted_iota(jnp.int32, (1, lon // fine), 1) * fine, lon)
    cos_b, sin_b = wave_trig(wave, lax.broadcasted_iota(jnp.int32, (1, fine), 1), lon)
    first = jnp.where(part == 0, cos_a, sin_a) * scale
    second = jnp.where(part == 0, -sin_a, cos_a) * scale
    first, second, cos_b, sin_b = lax.optimization_barrier((first, second, cos_b, sin_b))
    value = first[:, :, None] * cos_b[:, None, :] + second[:, :, None] * sin_b[:, None, :]
    return lax.optimization_barrier(value.reshape(rows, lon).astype(jnp.bfloat16))


def split_kernel(halves, me_ref, *refs):
    ins, outs, pieces_ref = refs[:halves], refs[halves:-1], refs[-1]
    step, levels, lon = ins[0].shape
    lines = step * levels
    to = lax.broadcasted_iota(jnp.int32, (lines, lines), 0)
    at = lax.broadcasted_iota(jnp.int32, (lines, lines), 1)
    move = (to % step * levels + to // step == at).astype(jnp.bfloat16)
    for h in range(halves):
        moved = jnp.dot(
            move, ins[h][...].reshape(lines, lon), preferred_element_type=jnp.float32
        ).astype(jnp.bfloat16)
        for e in range(levels):
            pieces_ref[e * halves + h] = moved[e * step : (e + 1) * step]
    for s, out_ref in enumerate(outs):
        out_ref[...] = pieces_ref[me_ref[0] ^ s]


def split(field, me, members):
    rows, levels, lon = field.shape
    halves = members // levels
    piece = rows // halves
    step = 16 if piece % 16 == 0 else piece
    blocks = piece // step
    return pl.pallas_call(
        lambda *refs: split_kernel(halves, *refs),
        out_shape=[jax.ShapeDtypeStruct((piece, lon), jnp.bfloat16)] * members,
        grid_spec=pltpu.PrefetchScalarGridSpec(
            num_scalar_prefetch=1,
            grid=(blocks,),
            in_specs=[
                pl.BlockSpec((step, levels, lon), lambda i, s, h=h: (h * blocks + i, 0, 0))
                for h in range(halves)
            ],
            out_specs=[pl.BlockSpec((step, lon), lambda i, s: (i, 0))] * members,
            scratch_shapes=[pltpu.VMEM((members, step, lon), jnp.bfloat16)],
        ),
        name="split",
    )(me.reshape(1), *[field] * halves)


def score_kernel(members, slots_ref, *refs):
    truth_ref, table_hbm, out_ref, lines_ref, table_ref, arrived = refs[members:]
    copy = pltpu.make_async_copy(table_hbm, table_ref, arrived)
    pl.when(pl.program_id(0) == 0)(copy.start)
    step, lon = truth_ref.shape
    padded = lines_ref.shape[0] // members
    inverse = 1.0 / (members - 1)
    lanes = 256 if lon % 256 == 0 else lon
    row = pl.program_id(0) * step
    one, minus, zero = (jnp.full((step, lanes), v, jnp.bfloat16) for v in (1, -1, 0))

    def sign(a, b):
        return jnp.where(a > b, one, jnp.where(a < b, minus, zero))

    def columns(c, carry):
        cols = pl.ds(pl.multiple_of(c * lanes, lanes), lanes)
        values = [refs[i][:, cols] for i in range(members)]
        truth = truth_ref[:, cols]
        ranks = [zero] * members
        for i in range(members):
            for j in range(i):
                s = sign(values[i], values[j])
                ranks[i] = ranks[i] + s
                ranks[j] = ranks[j] - s
        for i in range(members):
            grad = sign(values[i], truth).astype(jnp.float32)
            grad = grad - ranks[i].astype(jnp.float32) * inverse
            place = pl.multiple_of(slots_ref[i] * padded + row, 16)
            lines_ref[pl.ds(place, step), cols] = grad.astype(jnp.bfloat16)
        return carry

    lax.fori_loop(0, lon // lanes, columns, 0)

    @pl.when(pl.program_id(0) == pl.num_programs(0) - 1)
    def _():
        copy.wait()
        coeffs = lax.dot_general(
            table_ref[...],
            lines_ref[...],
            (((1,), (1,)), ((), ())),
            preferred_element_type=jnp.float32,
        )
        out_ref[...] = coeffs.reshape(out_ref.shape).astype(jnp.bfloat16)


def score_coeffs(blocks, slots, truth, table):
    members = len(blocks)
    piece, lon = truth.shape
    cols = table.shape[0]
    step = 16 if piece % 16 == 0 else piece
    padded = -(-piece // 16) * 16
    spec = pl.BlockSpec((step, lon), lambda i, s: (i, 0))
    coeffs = pl.pallas_call(
        lambda *refs: score_kernel(members, *refs),
        out_shape=jax.ShapeDtypeStruct((cols // 4, 4, members * padded), jnp.bfloat16),
        grid_spec=pltpu.PrefetchScalarGridSpec(
            num_scalar_prefetch=1,
            grid=(piece // step,),
            in_specs=[spec] * (members + 1) + [pl.BlockSpec(memory_space=pltpu.HBM)],
            out_specs=pl.BlockSpec((cols // 4, 4, members * padded), lambda i, s: (0, 0, 0)),
            scratch_shapes=[
                pltpu.VMEM((members * padded, lon), jnp.bfloat16),
                pltpu.VMEM((cols, lon), jnp.bfloat16),
                pltpu.SemaphoreType.DMA,
            ],
        ),
        compiler_params=pltpu.CompilerParams(vmem_limit_bytes=60 * 2**20),
        name="score",
    )(slots, *blocks, truth, table)
    coeffs = coeffs.reshape(cols // 4, 4, members, padded)[..., :piece]
    return coeffs.reshape(cols // 4, 4, members * piece)


def grid_kernel(rows, levels, coeffs_ref, table_ref, *refs):
    out_ref, lines_ref = refs[-2:]
    lines = rows * levels

    @pl.when(pl.program_id(0) == 0)
    def _():
        to = lax.broadcasted_iota(jnp.int32, (lines, lines), 0)
        at = lax.broadcasted_iota(jnp.int32, (lines, lines), 1)
        move = (to % levels * rows + to // levels == at).astype(jnp.bfloat16)
        moved = lax.dot_general(
            move,
            coeffs_ref[...].reshape(-1, lines),
            (((1,), (1,)), ((), ())),
            preferred_element_type=jnp.float32,
        )
        lines_ref[...] = moved.astype(jnp.bfloat16)

    grid = jnp.dot(lines_ref[...], table_ref[...], preferred_element_type=jnp.float32)
    grid = grid.reshape(rows, levels, -1)
    if len(refs) == 3:
        grid = grid + refs[0][...].astype(jnp.float32)
    out_ref[...] = grid.astype(jnp.bfloat16)


def to_grid(coeffs, table, added, rows, levels):
    cols, lon = table.shape
    step = 512 if lon % 512 == 0 else lon
    block = pl.BlockSpec((rows, levels, step), lambda i: (0, 0, i))
    return pl.pallas_call(
        lambda *refs: grid_kernel(rows, levels, *refs),
        out_shape=jax.ShapeDtypeStruct((rows, levels, lon), jnp.bfloat16),
        grid=(lon // step,),
        in_specs=[
            pl.BlockSpec((cols // 4, 4, rows * levels), lambda i: (0, 0, 0)),
            pl.BlockSpec((cols, step), lambda i: (0, i)),
        ]
        + [block] * (added is not None),
        out_specs=block,
        scratch_shapes=[pltpu.VMEM((rows * levels, cols), jnp.bfloat16)],
        name="grid",
    )(coeffs.reshape(cols // 4, 4, rows * levels), table, *([added] if added is not None else []))


def solution(mesh):
    members, lats = mesh.shape["member"], mesh.shape["lat"]
    both = ("lat", "member")

    def work(start, forcing, outlook, truth, basis, attenuation):
        _, rows, levels, lon = start.shape
        waves, lat_rows, _ = basis.shape
        per = -(-waves // members)
        halves = members // levels
        piece = rows // halves
        me = lax.axis_index("member")

        sent = split(outlook[0], me, members)
        sent, start = lax.optimization_barrier((sent, start))
        blocks, slots = [sent[0]], [me]
        for s in range(1, members):
            blocks.append(
                lax.ppermute(sent[s], "member", [(a, a ^ s) for a in range(members)])
            )
            slots.append(me ^ s)
        truth_here = lax.dynamic_slice(
            truth, (me % halves * piece, me // halves, 0), (piece, 1, lon)
        ).reshape(piece, lon)

        owner = jnp.arange(lats * members)
        table = fourier_rows(lon, owner // members, owner % members, per, waves)
        mine = jnp.pad(basis, ((0, members * per - waves), (0, 0), (0, 0)))
        mine = lax.dynamic_slice_in_dim(mine, me * per, per, 0)

        def lines_coeffs(lines):
            coeffs = lax.dot_general(
                table, lines, (((1,), (1,)), ((), ())), preferred_element_type=jnp.float32
            ).astype(jnp.bfloat16)
            return coeffs

        def to_waves(coeffs):
            coeffs = coeffs.reshape(lats * members, per // 2, 4, -1)
            return lax.all_to_all(coeffs, both, 0, 0, tiled=True)

        def legendre(coeffs):
            spectra = jnp.einsum(
                "jln,jcl->jcn", mine, coeffs, preferred_element_type=jnp.float32
            )
            spectra = (spectra * attenuation).astype(jnp.bfloat16)
            back = jnp.einsum(
                "jln,jcn->jcl", mine, spectra, preferred_element_type=jnp.float32
            ).astype(jnp.bfloat16)
            back = back.reshape(per, members, levels, 2, lats, rows)
            back = back.transpose(4, 1, 0, 3, 2, 5)
            return back.reshape(lats * members, per // 2, 4, levels * rows)

        lines = start[0].transpose(1, 0, 2).reshape(levels * rows, lon)
        received = to_waves(lines_coeffs(lines))
        score = score_coeffs(blocks, jnp.stack(slots), truth_here, table)
        received, score = lax.optimization_barrier((received, score))
        score = to_waves(score)
        coeffs = received.reshape(lats, members, per, 2, levels, rows)
        coeffs = coeffs.transpose(2, 1, 4, 3, 0, 5).reshape(per, members * levels * 2, lat_rows)
        state = to_waves(legendre(coeffs))

        coeffs = score.reshape(lats, levels, halves, per, 2, members, piece)
        coeffs = coeffs.transpose(3, 5, 1, 4, 0, 2, 6)
        coeffs = coeffs.reshape(per, members * levels * 2, lat_rows)
        score = to_waves(legendre(coeffs))
        advanced = to_grid(state, table, forcing[0], rows, levels)
        carried = to_grid(score, table, None, rows, levels)
        return advanced[None], carried[None]

    return jax.shard_map(
        work,
        mesh=mesh,
        in_specs=(
            P("member", "lat", None, None),
            P("member", "lat", None, None),
            P("member", "lat", None, None),
            P("lat", None, None),
            P("lat", None, None),
            P(),
        ),
        out_specs=(P("member", "lat", None, None), P("member", "lat", None, None)),
        check_vma=False,
    )
```

```python
import math

import jax
import jax.numpy as jnp
from jax import lax
from jax.experimental import pallas as pl
from jax.experimental.pallas import tpu as pltpu
from jax.sharding import PartitionSpec as P


def wave_trig(wave, place, lon):
    phase = (wave * place % lon).astype(jnp.float32) * (2.0 * math.pi / lon)
    return jnp.cos(phase), jnp.sin(phase)


def fourier_rows(lon, lat, member, per, waves):
    fine = math.gcd(lon, 128)
    row = lax.broadcasted_iota(jnp.int32, (lat.shape[0], per * 2, 1), 1)
    part = (row % 2).reshape(-1, 1)
    place = (member[:, None, None] * per + row // 2).reshape(-1, 1)
    wave = place + jnp.repeat(lat * waves, per * 2)[:, None]
    rows = wave.shape[0]
    scale = jnp.where(place < waves, math.sqrt(2.0 / lon), 0.0)
    cos_a, sin_a = wave_trig(wave, lax.broadcasted_iota(jnp.int32, (1, lon // fine), 1) * fine, lon)
    cos_b, sin_b = wave_trig(wave, lax.broadcasted_iota(jnp.int32, (1, fine), 1), lon)
    first = jnp.where(part == 0, cos_a, sin_a) * scale
    second = jnp.where(part == 0, -sin_a, cos_a) * scale
    first, second, cos_b, sin_b = lax.optimization_barrier((first, second, cos_b, sin_b))
    value = first[:, :, None] * cos_b[:, None, :] + second[:, :, None] * sin_b[:, None, :]
    return lax.optimization_barrier(value.reshape(rows, lon).astype(jnp.bfloat16))


def split_kernel(halves, me_ref, *refs):
    ins, outs, pieces_ref = refs[:halves], refs[halves:-1], refs[-1]
    step, levels, lon = ins[0].shape
    lines = step * levels
    to = lax.broadcasted_iota(jnp.int32, (lines, lines), 0)
    at = lax.broadcasted_iota(jnp.int32, (lines, lines), 1)
    move = (to % step * levels + to // step == at).astype(jnp.bfloat16)
    for h in range(halves):
        moved = jnp.dot(
            move, ins[h][...].reshape(lines, lon), preferred_element_type=jnp.float32
        ).astype(jnp.bfloat16)
        for e in range(levels):
            pieces_ref[e * halves + h] = moved[e * step : (e + 1) * step]
    for s, out_ref in enumerate(outs):
        out_ref[...] = pieces_ref[me_ref[0] ^ s]


def split(field, me, members):
    rows, levels, lon = field.shape
    halves = members // levels
    piece = rows // halves
    step = 16 if piece % 16 == 0 else piece
    blocks = piece // step
    return pl.pallas_call(
        lambda *refs: split_kernel(halves, *refs),
        out_shape=[jax.ShapeDtypeStruct((piece, lon), jnp.bfloat16)] * members,
        grid_spec=pltpu.PrefetchScalarGridSpec(
            num_scalar_prefetch=1,
            grid=(blocks,),
            in_specs=[
                pl.BlockSpec((step, levels, lon), lambda i, s, h=h: (h * blocks + i, 0, 0))
                for h in range(halves)
            ],
            out_specs=[pl.BlockSpec((step, lon), lambda i, s: (i, 0))] * members,
            scratch_shapes=[pltpu.VMEM((members, step, lon), jnp.bfloat16)],
        ),
        name="split",
    )(me.reshape(1), *[field] * halves)


def score_kernel(members, slots_ref, *refs):
    truth_ref, table_hbm, out_ref, lines_ref, table_ref, arrived = refs[members:]
    copy = pltpu.make_async_copy(table_hbm, table_ref, arrived)
    pl.when(pl.program_id(0) == 0)(copy.start)
    step, lon = truth_ref.shape
    padded = lines_ref.shape[0] // members
    inverse = 1.0 / (members - 1)
    lanes = 256 if lon % 256 == 0 else lon
    row = pl.program_id(0) * step
    one, minus, zero = (jnp.full((step, lanes), v, jnp.bfloat16) for v in (1, -1, 0))

    def sign(a, b):
        return jnp.where(a > b, one, jnp.where(a < b, minus, zero))

    def columns(c, carry):
        cols = pl.ds(pl.multiple_of(c * lanes, lanes), lanes)
        values = [refs[i][:, cols] for i in range(members)]
        truth = truth_ref[:, cols]
        ranks = [zero] * members
        for i in range(members):
            for j in range(i):
                s = sign(values[i], values[j])
                ranks[i] = ranks[i] + s
                ranks[j] = ranks[j] - s
        for i in range(members):
            grad = sign(values[i], truth).astype(jnp.float32)
            grad = grad - ranks[i].astype(jnp.float32) * inverse
            place = pl.multiple_of(slots_ref[i] * padded + row, 16)
            lines_ref[pl.ds(place, step), cols] = grad.astype(jnp.bfloat16)
        return carry

    lax.fori_loop(0, lon // lanes, columns, 0)

    @pl.when(pl.program_id(0) == pl.num_programs(0) - 1)
    def _():
        copy.wait()
        coeffs = lax.dot_general(
            table_ref[...],
            lines_ref[...],
            (((1,), (1,)), ((), ())),
            preferred_element_type=jnp.float32,
        )
        out_ref[...] = coeffs.reshape(out_ref.shape).astype(jnp.bfloat16)


def score_coeffs(blocks, slots, truth, table):
    members = len(blocks)
    piece, lon = truth.shape
    cols = table.shape[0]
    step = 16 if piece % 16 == 0 else piece
    padded = -(-piece // 16) * 16
    spec = pl.BlockSpec((step, lon), lambda i, s: (i, 0))
    coeffs = pl.pallas_call(
        lambda *refs: score_kernel(members, *refs),
        out_shape=jax.ShapeDtypeStruct((cols // 4, 4, members * padded), jnp.bfloat16),
        grid_spec=pltpu.PrefetchScalarGridSpec(
            num_scalar_prefetch=1,
            grid=(piece // step,),
            in_specs=[spec] * (members + 1) + [pl.BlockSpec(memory_space=pltpu.HBM)],
            out_specs=pl.BlockSpec((cols // 4, 4, members * padded), lambda i, s: (0, 0, 0)),
            scratch_shapes=[
                pltpu.VMEM((members * padded, lon), jnp.bfloat16),
                pltpu.VMEM((cols, lon), jnp.bfloat16),
                pltpu.SemaphoreType.DMA,
            ],
        ),
        compiler_params=pltpu.CompilerParams(vmem_limit_bytes=60 * 2**20),
        name="score",
    )(slots, *blocks, truth, table)
    coeffs = coeffs.reshape(cols // 4, 4, members, padded)[..., :piece]
    return coeffs.reshape(cols // 4, 4, members * piece)


def grid_kernel(rows, levels, coeffs_ref, table_ref, *refs):
    out_ref, lines_ref = refs[-2:]
    lines = rows * levels

    @pl.when(pl.program_id(0) == 0)
    def _():
        to = lax.broadcasted_iota(jnp.int32, (lines, lines), 0)
        at = lax.broadcasted_iota(jnp.int32, (lines, lines), 1)
        move = (to % levels * rows + to // levels == at).astype(jnp.bfloat16)
        moved = lax.dot_general(
            move,
            coeffs_ref[...].reshape(-1, lines),
            (((1,), (1,)), ((), ())),
            preferred_element_type=jnp.float32,
        )
        lines_ref[...] = moved.astype(jnp.bfloat16)

    grid = jnp.dot(lines_ref[...], table_ref[...], preferred_element_type=jnp.float32)
    grid = grid.reshape(rows, levels, -1)
    if len(refs) == 3:
        grid = grid + refs[0][...].astype(jnp.float32)
    out_ref[...] = grid.astype(jnp.bfloat16)


def to_grid(coeffs, table, added, rows, levels):
    cols, lon = table.shape
    step = 1280 if lon % 1280 == 0 else lon
    block = pl.BlockSpec((rows, levels, step), lambda i: (0, 0, i))
    return pl.pallas_call(
        lambda *refs: grid_kernel(rows, levels, *refs),
        out_shape=jax.ShapeDtypeStruct((rows, levels, lon), jnp.bfloat16),
        grid=(lon // step,),
        in_specs=[
            pl.BlockSpec((cols // 4, 4, rows * levels), lambda i: (0, 0, 0)),
            pl.BlockSpec((cols, step), lambda i: (0, i)),
        ]
        + [block] * (added is not None),
        out_specs=block,
        scratch_shapes=[pltpu.VMEM((rows * levels, cols), jnp.bfloat16)],
        compiler_params=pltpu.CompilerParams(vmem_limit_bytes=56 * 2**20),
        name="grid",
    )(coeffs.reshape(cols // 4, 4, rows * levels), table, *([added] if added is not None else []))


def solution(mesh):
    members, lats = mesh.shape["member"], mesh.shape["lat"]
    both = ("lat", "member")

    def work(start, forcing, outlook, truth, basis, attenuation):
        _, rows, levels, lon = start.shape
        waves, lat_rows, _ = basis.shape
        per = -(-waves // members)
        halves = members // levels
        piece = rows // halves
        me = lax.axis_index("member")

        sent = split(outlook[0], me, members)
        sent, start = lax.optimization_barrier((sent, start))
        blocks, slots = [sent[0]], [me]
        for s in range(members - 1, 0, -1):
            blocks.append(
                lax.ppermute(sent[s], "member", [(a, a ^ s) for a in range(members)])
            )
            slots.append(me ^ s)
        truth_here = lax.dynamic_slice(
            truth, (me % halves * piece, me // halves, 0), (piece, 1, lon)
        ).reshape(piece, lon)

        owner = jnp.arange(lats * members)
        table = fourier_rows(lon, owner // members, owner % members, per, waves)
        mine = jnp.pad(basis, ((0, members * per - waves), (0, 0), (0, 0)))
        mine = lax.dynamic_slice_in_dim(mine, me * per, per, 0)

        def lines_coeffs(lines):
            coeffs = lax.dot_general(
                table, lines, (((1,), (1,)), ((), ())), preferred_element_type=jnp.float32
            ).astype(jnp.bfloat16)
            return coeffs

        def to_waves(coeffs):
            coeffs = coeffs.reshape(lats * members, per // 2, 4, -1)
            return lax.all_to_all(coeffs, both, 0, 0, tiled=True)

        def legendre(coeffs):
            spectra = jnp.einsum(
                "jln,jcl->jcn", mine, coeffs, preferred_element_type=jnp.float32
            )
            spectra = (spectra * attenuation).astype(jnp.bfloat16)
            back = jnp.einsum(
                "jln,jcn->jcl", mine, spectra, preferred_element_type=jnp.float32
            ).astype(jnp.bfloat16)
            back = back.reshape(per, members, levels, 2, lats, rows)
            back = back.transpose(4, 1, 0, 3, 2, 5)
            return back.reshape(lats * members, per // 2, 4, levels * rows)

        lines = start[0].transpose(1, 0, 2).reshape(levels * rows, lon)
        received = to_waves(lines_coeffs(lines))
        score = score_coeffs(blocks, jnp.stack(slots), truth_here, table)
        received, score = lax.optimization_barrier((received, score))
        score = to_waves(score)
        coeffs = received.reshape(lats, members, per, 2, levels, rows)
        coeffs = coeffs.transpose(2, 1, 4, 3, 0, 5).reshape(per, members * levels * 2, lat_rows)
        state = to_waves(legendre(coeffs))

        coeffs = score.reshape(lats, levels, halves, per, 2, members, piece)
        coeffs = coeffs.transpose(3, 5, 1, 4, 0, 2, 6)
        coeffs = coeffs.reshape(per, members * levels * 2, lat_rows)
        score = to_waves(legendre(coeffs))
        advanced = to_grid(state, table, forcing[0], rows, levels)
        carried = to_grid(score, table, None, rows, levels)
        return advanced[None], carried[None]

    return jax.shard_map(
        work,
        mesh=mesh,
        in_specs=(
            P("member", "lat", None, None),
            P("member", "lat", None, None),
            P("member", "lat", None, None),
            P("lat", None, None),
            P("lat", None, None),
            P(),
        ),
        out_specs=(P("member", "lat", None, None), P("member", "lat", None, None)),
        check_vma=False,
    )
```
